256 devices in a mesh: ta: 8 (over x, z_lo), sa: 32 (over z_hi, y, core).
Axes of the slice: x: 4, y: 4, z: 8 (z_hi: 4, z_lo: 2; z = z_hi * 2 + z_lo), core: 2. Of those that a mesh axis runs over, the one named last changes fastest.
Arguments:
- eigvecs: bfloat16 [48, 2, 3, 13824, 128], P('ta', None, None, 'sa'), may hold values from -0.0390625 to 0.0390625
- solutions: bfloat16 [48, 2, 3, 13824, 128], P('ta', None, None, 'sa'), may hold values from -6 to 6
Outputs:
- tau: float32 [48, 2, 128, 128], P('ta', None, 'sa')
- corr: float32 [48], replicated
The draws below stay inside these ranges and needn't reach their ends.
All inputs are finite; a program needn't handle non-finite values.
Results may differ from the reference program's by a relative error of at most 0.0003.
Values sent between devices are 32-bit elements; how exact they have to be, the bound alone decides.
A program may use at most 64 MiB of HBM per device.

```python
import jax
import jax.numpy as jnp
from jax import lax

NEV = 128
NB = 128
NT = 48
SITES = 13824


def strengthened(entries, stream_key, source, target, parts, factor):
    def block_of(position):
        return (jnp.arange(entries.shape[position]) // (entries.shape[position] // parts)).reshape((-1,) + (1,) * (entries.ndim - 1 - position))

    near = jax.random.permutation(stream_key, parts)[block_of(target)]
    second = (block_of(target) + parts // 2) % parts
    return jnp.where((block_of(source) == near) | (block_of(source) == second), factor * entries, entries)


def steps_of(own_key, dims, split, smallest, top_value):
    loudness = 1.0
    for position, blocks in split:
        draws = jax.random.uniform(jax.random.fold_in(jax.random.fold_in(own_key, 6), position), (blocks,), jnp.float32, smallest / len(split), top_value / len(split))
        loudness = loudness * jnp.repeat(jnp.exp(draws), dims[position] // blocks).reshape((-1,) + (1,) * (len(dims) - 1 - position))
    return loudness


def bell_draw(stream_key, extent, deviation, reach, cuts=(), kind=jnp.bfloat16):
    drawn = deviation * jax.random.normal(stream_key, extent, jnp.float32)
    if cuts:
        drawn = drawn * steps_of(stream_key, extent, cuts, -0.22, 0.18)
    return jnp.clip(drawn, -reach, reach).astype(kind)


def gaussian_with(own_key, dims, width, bound, shards, heavy, dtype=jnp.bfloat16):
    drawn = width * jax.random.normal(own_key, dims, jnp.float32)
    if shards:
        drawn = drawn * steps_of(own_key, dims, shards, -0.22, 0.18)
    return jnp.clip(strengthened(drawn, jax.random.fold_in(own_key, 3), *heavy), -bound, bound).astype(dtype)


def setup_inputs(seed: int = 0) -> dict:
    splits = jax.random.split(jax.random.key(seed), 3)
    return {
        "eigvecs": gaussian_with(splits[0], (NT, 2, 3, SITES, NEV), (6 * SITES) ** -0.5, 0.0390625, ((0, 8), (3, 32)), (3, 4, 32, 2.75)),
        "solutions": bell_draw(splits[1], (NT, 2, 3, SITES, NB), 1.0, 6.0, ((0, 8), (3, 32))),
    }


def contract(left, right):
    return lax.dot_general(left, right, (((0,), (0,)), ((), ())), preferred_element_type=jnp.float32)


def one_slice(pair):
    vecs, sols = pair
    vec_re = vecs[0].reshape(-1, vecs.shape[-1])
    vec_im = vecs[1].reshape(-1, vecs.shape[-1])
    sol_re = sols[0].reshape(-1, sols.shape[-1])
    sol_im = sols[1].reshape(-1, sols.shape[-1])
    real_part = contract(vec_re, sol_re) + contract(vec_im, sol_im)
    imag_part = contract(vec_re, sol_im) - contract(vec_im, sol_re)
    return jnp.stack([real_part, imag_part], 0)


def reference(eigvecs, solutions):
    tau = lax.map(one_slice, (eigvecs, solutions))
    corr = jnp.sum(tau * tau, axis=(1, 2, 3)) / (2.0 * NEV * NB)
    return tau, corr
```

```python
import functools

import jax
import jax.numpy as jnp
from jax import lax
from jax.experimental import pallas as pl
from jax.experimental.pallas import tpu as pltpu
from jax.sharding import PartitionSpec as P

MESH = pl.DeviceIdType.MESH
X, Y, ZH, ZL, CORES = 4, 4, 4, 2, 2
Z = ZH * ZL
NT = 6
TG = 1
NG = NT // TG
BARRIER_AFTER = 3
F32 = jnp.float32


def position():
    ta, sa = lax.axis_index("ta"), lax.axis_index("sa")
    x, zl = lax.div(ta, ZL), lax.rem(ta, ZL)
    zh, y, core = lax.div(sa, Y * CORES), lax.rem(lax.div(sa, CORES), Y), lax.rem(sa, CORES)
    return x, y, zh, zl, core


def device(x, y, zh, zl, core):
    return (x * ZL + zl, (zh * Y + y) * CORES + core)


def kernel(
    scale, v_hbm, p_hbm, tau_ref, corr_ref,
    vbuf, pbuf, csend, keep, crecv, ysend, yrecv, zsend, zrecv, row1, recv1, row2, recv2,
    in_sem, csem_s, csem_r, ysem_s, ysem_r, zsem_s, zsem_r, nsem,
):
    x, y, zh, zl, core = position()
    z = zh * ZL + zl

    def load(t):
        return [
            pltpu.make_async_copy(v_hbm.at[t], vbuf.at[t], in_sem.at[t, 0]),
            pltpu.make_async_copy(p_hbm.at[t], pbuf.at[t], in_sem.at[t, 1]),
        ]

    peers1, peers2 = [], []
    for dz in range(Z):
        for dc in range(CORES):
            if dz or dc:
                zz = lax.rem(z + dz, Z)
                peers1.append((dz * CORES + dc, device(x, y, lax.div(zz, ZL), lax.rem(zz, ZL), lax.rem(core + dc, CORES))))
    for dx in range(X):
        for dy in range(Y):
            if dx or dy:
                peers2.append((dx * Y + dy, device(lax.rem(x + dx, X), lax.rem(y + dy, Y), zh, zl, core)))

    for copy in load(0):
        copy.start()
    barrier = pltpu.get_barrier_semaphore()
    for _, peer in peers1 + peers2:
        pl.semaphore_signal(barrier, inc=1, device_id=peer, device_id_type=MESH)
    for t in range(1, NT):
        for copy in load(t):
            copy.start()

    def remote(src, dst, send, recv, peer):
        return pltpu.make_async_remote_copy(
            src_ref=src, dst_ref=dst, send_sem=send, recv_sem=recv, device_id=peer, device_id_type=MESH
        )

    def to_core(t):
        return remote(csend.at[t], crecv.at[t], csem_s.at[t], csem_r.at[t], device(x, y, zh, zl, 1 - core))

    low = lax.broadcasted_iota(jnp.int32, (128, 128), 0) % 8 < 4
    first = core == 0
    for t in range(NT):
        for copy in load(t):
            copy.wait()
        v = jnp.concatenate([vbuf[t, 0], vbuf[t, 1]], axis=1)
        p = jnp.concatenate([pbuf[t, 0], pbuf[t, 1]], axis=1)
        o = lax.dot_general(v, p, (((0,), (0,)), ((), ())), preferred_element_type=F32)
        re = o[:128, :128] + o[128:, 128:]
        im = o[:128, 128:] - o[128:, :128]
        for0 = jnp.where(low, re, pltpu.roll(im, 4, 0))
        for1 = jnp.where(low, pltpu.roll(re, 124, 0), im)
        mine = jnp.where(first, for0, for1)
        other = jnp.where(first, for1, for0)
        csend[t] = other.reshape(ZH * Y, 8, 128)
        keep[t] = mine.reshape(ZH * Y, 8, 128)
        if t == BARRIER_AFTER:
            pl.semaphore_wait(barrier, len(peers1) + len(peers2))
            for s in range(t + 1):
                to_core(s).start()
        elif t > BARRIER_AFTER:
            to_core(t).start()

    def to_y(g, d):
        yy = lax.rem(y + d, Y)
        return remote(
            ysend.at[g, yy], yrecv.at[g, d - 1], ysem_s.at[g, d - 1], ysem_r.at[g, d - 1], device(x, yy, zh, zl, core)
        )

    def to_z(g, d):
        zz = lax.rem(zh + d, ZH)
        return remote(
            zsend.at[g, zz], zrecv.at[g, d - 1], zsem_s.at[g, d - 1], zsem_r.at[g, d - 1], device(x, y, zz, zl, core)
        )

    for g in range(NG):
        for i in range(TG):
            t = g * TG + i
            to_core(t).wait_recv()
            total = (keep[t] + crecv[t]).reshape(ZH, Y, 8, 128)
            for yy in range(Y):
                ysend[g, yy, i] = total[:, yy]
        for d in (2, 1, 3):
            to_y(g, d).start()
    for g in range(NG):
        for d in (1, 3, 2):
            to_y(g, d).wait_recv()
        total = ysend[g, y] + yrecv[g, 0] + yrecv[g, 1] + yrecv[g, 2]
        for zz in range(ZH):
            zsend[g, zz] = total[:, zz]
        for d in (2, 1, 3):
            to_z(g, d).start()
    lane = lax.broadcasted_iota(jnp.int32, (1, 128), 1)
    slot = (x * ZL + zl) * NT
    row = jnp.zeros((1, 128), F32)
    for g in range(NG):
        for d in (1, 3, 2):
            to_z(g, d).wait_recv()
        total = zsend[g, zh] + zrecv[g, 0] + zrecv[g, 1] + zrecv[g, 2]
        for i in range(TG):
            t = g * TG + i
            tau_ref[t] = total[i]
            norm = jnp.sum(total[i] * total[i], axis=(0, 1), keepdims=True)
            row = row + jnp.where(lane == slot + t, norm, 0.0)

    def share(row, own, recv, peers, stage):
        own[...] = row
        recv[0:1] = row
        for k, peer in peers:
            remote(own, recv.at[pl.ds(k, 1)], nsem.at[stage, 0], nsem.at[stage, 1], peer).start()
        rest = pltpu.make_async_copy(recv.at[pl.ds(1, len(peers))], recv.at[pl.ds(1, len(peers))], nsem.at[stage, 1])
        rest.wait()
        return jnp.sum(recv[...], axis=0, keepdims=True)

    row = share(row, row1, recv1, peers1, 0)
    row = share(row, row2, recv2, peers2, 1)
    corr_ref[...] = row * scale

    for stage, recv, peers in ((0, recv1, peers1), (1, recv2, peers2)):
        pltpu.make_async_copy(recv.at[pl.ds(1, len(peers))], recv.at[pl.ds(1, len(peers))], nsem.at[stage, 0]).wait()
    for t in range(NT):
        to_core(t).wait_send()
    for g in range(NG):
        for d in range(1, Y):
            to_y(g, d).wait_send()
        for d in range(1, ZH):
            to_z(g, d).wait_send()


def per_device(eigvecs, solutions):
    rows = eigvecs.shape[2] * eigvecs.shape[3]
    v = eigvecs.reshape(NT, 2, rows, 128)
    p = solutions.reshape(NT, 2, rows, 128)
    vmem = pl.BlockSpec(memory_space=pltpu.VMEM)
    hbm = pl.BlockSpec(memory_space=pltpu.HBM)
    tau, corr = pl.pallas_call(
        functools.partial(kernel, 1.0 / (2.0 * 128 * 128)),
        out_shape=(jax.ShapeDtypeStruct((NT, 8, 128), F32), jax.ShapeDtypeStruct((1, 128), F32)),
        in_specs=[hbm, hbm],
        out_specs=(vmem, vmem),
        scratch_shapes=[
            pltpu.VMEM((NT, 2, rows, 128), jnp.bfloat16),
            pltpu.VMEM((NT, 2, rows, 128), jnp.bfloat16),
            pltpu.VMEM((NT, ZH * Y, 8, 128), F32),
            pltpu.VMEM((NT, ZH * Y, 8, 128), F32),
            pltpu.VMEM((NT, ZH * Y, 8, 128), F32),
            pltpu.VMEM((NG, Y, TG, ZH, 8, 128), F32),
            pltpu.VMEM((NG, Y - 1, TG, ZH, 8, 128), F32),
            pltpu.VMEM((NG, ZH, TG, 8, 128), F32),
            pltpu.VMEM((NG, ZH - 1, TG, 8, 128), F32),
            pltpu.VMEM((1, 128), F32),
            pltpu.VMEM((Z * CORES, 128), F32),
            pltpu.VMEM((1, 128), F32),
            pltpu.VMEM((X * Y, 128), F32),
            pltpu.SemaphoreType.DMA((NT, 2)),
            pltpu.SemaphoreType.DMA((NT,)),
            pltpu.SemaphoreType.DMA((NT,)),
            pltpu.SemaphoreType.DMA((NG, Y - 1)),
            pltpu.SemaphoreType.DMA((NG, Y - 1)),
            pltpu.SemaphoreType.DMA((NG, ZH - 1)),
            pltpu.SemaphoreType.DMA((NG, ZH - 1)),
            pltpu.SemaphoreType.DMA((2, 2)),
        ],
        compiler_params=pltpu.CompilerParams(collective_id=0, has_side_effects=True, vmem_limit_bytes=60 * 1024 * 1024),
    )(v, p)
    return tau.reshape(NT, 2, 4, 128), corr[0, :48]


def solution(mesh):
    in_specs = (P("ta", None, None, "sa", None), P("ta", None, None, "sa", None))
    out_specs = (P("ta", None, "sa", None), P())
    return jax.shard_map(
        per_device, mesh=mesh, in_specs=in_specs, out_specs=out_specs, check_vma=False
    )
```
